32 devices in a mesh: frame: 16 (over z, y, x), row: 2 (over core).
Axes of the slice: x: 2, y: 2, z: 4, core: 2. Of those that a mesh axis runs over, the one named last changes fastest.
Arguments:
- footage: float32 [64, 1024, 1024], P('frame', 'row'), may hold values from -30 to 30
Outputs:
- coefficients: float32 [64, 1024, 1024], P('frame', 'row')
- energies: float32 [4, 10], replicated
The draws below stay inside these ranges and needn't reach their ends.
All inputs are finite; a program needn't handle non-finite values.
Results may differ from the reference program's by a relative error of at most 0.00007.
Values sent between devices are 32-bit elements; how exact they have to be, the bound alone decides.
A program may use at most 128 MiB of HBM per device.

```python
import math
from functools import partial
import jax
import jax.numpy as jnp
import numpy as np
from jax import lax

H = 1024
W = 1024
SLEVELS = 3
TLEVELS = 3
FRAMES = 64


def draw_footage(key, part):
    subkeys = jax.random.split(jax.random.fold_in(key, 7), 1)
    full_shape = (FRAMES, H, W)
    frame_ramp = jnp.arange(FRAMES, dtype=jnp.float32) / (FRAMES - 1)
    values = jnp.clip(jax.random.normal(subkeys[0], full_shape, jnp.float32), -5.0, 5.0)
    values = values * jnp.exp(math.log(3.0) * frame_ramp)[:, None, None]
    return values


def setup_inputs(seed: int = 0) -> dict:
    keys = jax.random.split(jax.random.key(seed), 2)
    return {
        "footage": draw_footage(jax.random.fold_in(keys[1], 71), 0),
    }


LIFT_ALPHA = -1.586134342
LIFT_BETA = -0.05298011854
LIFT_GAMMA = 0.8829110762
LIFT_DELTA = 0.4435068522
LIFT_ZETA = 1.149604398


def mirror_after(values, along):
    length = values.shape[along]
    return jnp.concatenate([lax.slice_in_dim(values, 1, length, axis=along), lax.slice_in_dim(values, length - 1, length, axis=along)], axis=along)


def mirror_before(values, along):
    length = values.shape[along]
    return jnp.concatenate([lax.slice_in_dim(values, 0, 1, axis=along), lax.slice_in_dim(values, 0, length - 1, axis=along)], axis=along)


def weave_axis(even_part, odd_part, along):
    stacked = jnp.stack([even_part, odd_part], axis=along + 1)
    new_shape = list(even_part.shape)
    new_shape[along] = new_shape[along] * 2
    return stacked.reshape(tuple(new_shape))


def lift_pair(even_part, odd_part, take_next, take_prev):
    odd_part = odd_part + LIFT_ALPHA * (even_part + take_next(even_part))
    even_part = even_part + LIFT_BETA * (take_prev(odd_part) + odd_part)
    odd_part = odd_part + LIFT_GAMMA * (even_part + take_next(even_part))
    even_part = even_part + LIFT_DELTA * (take_prev(odd_part) + odd_part)
    return even_part * LIFT_ZETA, odd_part * (1.0 / LIFT_ZETA)


def spatial(planes_in, levels, take_next, take_prev):
    row_axis = planes_in.ndim - 2
    col_axis = planes_in.ndim - 1
    low_cols, high_cols = lift_pair(planes_in[..., 0::2], planes_in[..., 1::2], partial(mirror_after, along=col_axis), partial(mirror_before, along=col_axis))
    combined = jnp.concatenate([low_cols, high_cols], axis=col_axis)
    low_rows, high_rows = lift_pair(combined[..., 0::2, :], combined[..., 1::2, :], take_next, take_prev)
    half_width = low_cols.shape[-1]
    coarse = low_rows[..., :half_width]
    if levels > 1:
        coarse = spatial(coarse, levels - 1, take_next, take_prev)
    upper_rows = weave_axis(coarse, low_rows[..., half_width:], col_axis)
    bottom = weave_axis(high_rows[..., :half_width], high_rows[..., half_width:], col_axis)
    return weave_axis(upper_rows, bottom, row_axis)


def temporal(planes_in, levels):
    even_part = planes_in[0::2]
    odd_part = planes_in[1::2]
    odd_part = odd_part - 0.5 * (even_part + mirror_after(even_part, 0))
    even_part = even_part + 0.25 * (mirror_before(odd_part, 0) + odd_part)
    if levels > 1:
        even_part = temporal(even_part, levels - 1)
    return weave_axis(even_part, odd_part, 0)


def level_of(number, ceiling):
    depth_now = 1
    while number % 2 == 0 and depth_now <= ceiling:
        number = number // 2
        depth_now = depth_now + 1
    return depth_now


def space_table(levels):
    period = 2 ** levels
    band_table = np.zeros((period * period, 3 * levels + 1), np.float32)
    for row_pos in range(period):
        for col_pos in range(period):
            row_level = level_of(row_pos, levels)
            col_level = level_of(col_pos, levels)
            finest = min(row_level, col_level)
            if finest > levels:
                column = 3 * levels
            elif row_level == col_level:
                column = 3 * (finest - 1) + 2
            elif row_level == finest:
                column = 3 * (finest - 1)
            else:
                column = 3 * (finest - 1) + 1
            band_table[row_pos * period + col_pos, column] = 1.0
    return band_table


def time_table(levels):
    period = 2 ** levels
    band_table = np.zeros((period, levels + 1), np.float32)
    for number in range(period):
        band_table[number, level_of(number, levels) - 1] = 1.0
    return band_table


def band_sums(coeffs, first_frame, levels_s, levels_t):
    period = 2 ** levels_s
    frame_count, row_count, col_count = coeffs.shape
    square = coeffs * coeffs
    pattern = square.reshape(frame_count, row_count // period, period, col_count // period, period).sum(axis=(1, 3))
    pattern = pattern.reshape(frame_count, period * period)
    per_frame = jnp.dot(pattern, jnp.asarray(space_table(levels_s), jnp.float32), precision=lax.Precision.HIGHEST)
    time_period = 2 ** levels_t
    position = (first_frame + jnp.arange(frame_count, dtype=jnp.int32)) % time_period
    onehot = (position[:, None] == jnp.arange(time_period, dtype=jnp.int32)[None, :]).astype(jnp.float32)
    frame_band = jnp.dot(onehot, jnp.asarray(time_table(levels_t), jnp.float32), precision=lax.Precision.HIGHEST)
    return jnp.dot(frame_band.T, per_frame, precision=lax.Precision.HIGHEST)


def band_means(totals, frames_all, rows_all, cols_all, levels_s, levels_t):
    space_share = space_table(levels_s).sum(0) / float((2 ** levels_s) ** 2)
    time_share = time_table(levels_t).sum(0) / float(2 ** levels_t)
    counts = float(frames_all) * float(rows_all) * float(cols_all) * np.outer(time_share, space_share)
    return totals / jnp.asarray(counts, jnp.float32)


def reference(footage):
    frames_all, rows_all, cols_all = footage.shape

    def picture_step(picture):
        return spatial(picture[None], SLEVELS, partial(mirror_after, along=1), partial(mirror_before, along=1))[0]

    planes = lax.map(picture_step, footage)
    block_rows = 8
    grouped = jnp.moveaxis(planes.reshape(frames_all, rows_all // block_rows, block_rows, cols_all), 1, 0)

    def time_step(row_block):
        return temporal(row_block, TLEVELS)

    temporal_out = lax.map(time_step, grouped)
    coeffs = jnp.moveaxis(temporal_out, 0, 1).reshape(frames_all, rows_all, cols_all)
    totals = band_sums(coeffs, 0, SLEVELS, TLEVELS)
    return coeffs, band_means(totals, frames_all, rows_all, cols_all, SLEVELS, TLEVELS)
```

```python
import functools

import jax
import jax.numpy as jnp
import numpy as np
from jax import lax
from jax.experimental import pallas as pl
from jax.experimental.pallas import tpu as pltpu
from jax.sharding import PartitionSpec as P

SLEVELS = 3
TLEVELS = 3
PERIOD = 2**SLEVELS
MARGIN = 4
GROUP = 4

LIFT_ALPHA = -1.586134342
LIFT_BETA = -0.05298011854
LIFT_GAMMA = 0.8829110762
LIFT_DELTA = 0.4435068522
LIFT_ZETA = 1.149604398
STEPS = (LIFT_ALPHA, LIFT_BETA, LIFT_GAMMA, LIFT_DELTA)
SCALES = 8 * SLEVELS
MASKS = SCALES + SLEVELS
MESH = pl.DeviceIdType.MESH


def level_of(number, ceiling):
    depth_now = 1
    while number % 2 == 0 and depth_now <= ceiling:
        number = number // 2
        depth_now = depth_now + 1
    return depth_now


def space_table(levels):
    period = 2**levels
    band_table = np.zeros((period * period, 3 * levels + 1), np.float32)
    for row_pos in range(period):
        for col_pos in range(period):
            row_level = level_of(row_pos, levels)
            col_level = level_of(col_pos, levels)
            finest = min(row_level, col_level)
            if finest > levels:
                column = 3 * levels
            elif row_level == col_level:
                column = 3 * (finest - 1) + 2
            elif row_level == finest:
                column = 3 * (finest - 1)
            else:
                column = 3 * (finest - 1) + 1
            band_table[row_pos * period + col_pos, column] = 1.0
    return band_table


def time_table(levels):
    period = 2**levels
    band_table = np.zeros((period, levels + 1), np.float32)
    for number in range(period):
        band_table[number, level_of(number, levels) - 1] = 1.0
    return band_table


def band_means(totals, frames_all, rows_all, cols_all, levels_s, levels_t):
    space_share = space_table(levels_s).sum(0) / float((2**levels_s) ** 2)
    time_share = time_table(levels_t).sum(0) / float(2**levels_t)
    counts = (
        float(frames_all) * float(rows_all) * float(cols_all) * np.outer(time_share, space_share)
    )
    return totals / jnp.asarray(counts, jnp.float32)


def shifted(block, axis, distance):
    devices = range(lax.axis_size(axis))
    route = [(i - distance, i) for i in devices if i - distance in devices]
    return lax.ppermute(block, axis, route)


def lane_table(width):
    lane = np.arange(width)
    table = np.zeros((MASKS + SLEVELS, width), np.float64)
    for level in range(SLEVELS):
        s = 2**level
        odd = lane % (2 * s) == s
        even = lane % (2 * s) == 0
        for step, factor in enumerate(STEPS):
            left = factor * (odd if step % 2 == 0 else even)
            right = left.copy()
            if step % 2 == 0:
                left[width - s], right[width - s] = 2 * factor, 0.0
            else:
                left[0], right[0] = 0.0, 2 * factor
            table[8 * level + 2 * step] = left
            table[8 * level + 2 * step + 1] = right
        table[SCALES + level] = np.where(even, LIFT_ZETA, np.where(odd, 1.0 / LIFT_ZETA, 1.0))
        table[MASKS + level] = lane % s == 0
    return table.astype(np.float32)


def spatial_kernel(tab_ref, x_ref, o_ref, buf):
    groups, width = buf.shape[1:]
    inner = groups - 2 * MARGIN
    row = lax.axis_index("row")
    at_top = row == 0
    at_bottom = row == lax.axis_size("row") - 1
    tiles = groups // 8

    for level in range(SLEVELS):
        s = 2**level
        source = x_ref.at[0] if level == 0 else buf

        def columns(i, carry, level=level, s=s, source=source):
            phase = (i // tiles) * s
            q = pl.ds(pl.multiple_of((i % tiles) * 8, 8), 8)
            x = source[phase, q, :]
            for step in range(4):
                k = 8 * level + 2 * step
                before = pltpu.roll(x, s, 1)
                after = pltpu.roll(x, width - s, 1)
                x = x + tab_ref[pl.ds(k, 1), :] * before + tab_ref[pl.ds(k + 1, 1), :] * after
            buf[phase, q, :] = x * tab_ref[pl.ds(SCALES + level, 1), :]
            return carry

        lax.fori_loop(0, (PERIOD // s) * tiles, columns, 0)

        def rows(i, carry, level=level, s=s):
            lanes = pl.ds(pl.multiple_of(i * 128, 128), 128)
            mask = tab_ref[pl.ds(MASKS + level, 1), lanes]
            x = {p: buf[p, :, lanes] for p in range(0, PERIOD, s)}
            index = lax.broadcasted_iota(jnp.int32, (groups, 128), 0)
            first = jnp.logical_and(index == MARGIN, at_top)
            last = jnp.logical_and(index == MARGIN + inner - 1, at_bottom)
            for step, factor in enumerate(STEPS):
                c = factor * mask
                if step % 2 == 0:
                    for p in range(s, PERIOD, 2 * s):
                        if p + s < PERIOD:
                            after = x[p + s]
                        else:
                            after = jnp.where(last, x[p - s], pltpu.roll(x[0], groups - 1, 0))
                        x[p] = x[p] + c * (x[p - s] + after)
                else:
                    for p in range(0, PERIOD, 2 * s):
                        if p > 0:
                            before = x[p - s]
                        else:
                            before = jnp.where(first, x[s], pltpu.roll(x[PERIOD - s], 1, 0))
                        x[p] = x[p] + c * (before + x[p + s])
            up = jnp.where(mask > 0, LIFT_ZETA, 1.0)
            down = jnp.where(mask > 0, 1.0 / LIFT_ZETA, 1.0)
            for p in x:
                low = p % (2 * s) == 0
                value = x[p] * (up if low else down)
                if low and level < SLEVELS - 1:
                    buf[p, :, lanes] = value
                else:
                    o_ref[0, p, :, lanes] = value[MARGIN : MARGIN + inner]
            return carry

        lax.fori_loop(0, width // 128, rows, 0)


def spatial(footage):
    frames, rows, width = footage.shape
    edge = MARGIN * PERIOD
    above = shifted(footage[:, -edge:], "row", 1)
    below = shifted(footage[:, :edge], "row", -1)
    groups = rows // PERIOD + 2 * MARGIN
    x = jnp.concatenate([above, footage, below], axis=1)
    x = x.reshape(frames, groups, PERIOD, width).transpose(0, 2, 1, 3)
    inner = rows // PERIOD
    table = jnp.asarray(lane_table(width))
    return pl.pallas_call(
        spatial_kernel,
        grid=(frames,),
        out_shape=jax.ShapeDtypeStruct((frames, PERIOD, inner, width), jnp.float32),
        in_specs=[
            pl.BlockSpec(table.shape, lambda i: (0, 0)),
            pl.BlockSpec((1, PERIOD, groups, width), lambda i: (i, 0, 0, 0)),
        ],
        out_specs=pl.BlockSpec((1, PERIOD, inner, width), lambda i: (i, 0, 0, 0)),
        scratch_shapes=[pltpu.VMEM((PERIOD, groups, width), jnp.float32)],
        compiler_params=pltpu.CompilerParams(vmem_limit_bytes=50 * 2**20),
    )(table, x)


def outgoing(f):
    o = {i: f[i] - 0.5 * (f[i - 1] + f[i + 1]) for i in range(1, 14, 2)}
    a = {i: f[i] + 0.25 * (o[i - 1] + o[i + 1]) for i in range(2, 13, 2)}
    p6 = a[6] - 0.5 * (a[4] + a[8])
    p10 = a[10] - 0.5 * (a[8] + a[12])
    b8 = a[8] + 0.25 * (p6 + p10)
    to_before = (f[0], o[1], a[2] - 0.5 * a[4])
    to_after = (
        f[15] - 0.5 * f[14],
        f[14] + 0.25 * o[13] - 0.5 * a[12],
        a[12] + 0.25 * p10 - 0.5 * b8,
    )
    return to_before, to_after


def temporal(f, before, after, is_first, is_last):
    o = {i: f[i] - 0.5 * (f[i - 1] + f[i + 1]) for i in range(1, 14, 2)}
    f16 = jnp.where(is_last, f[14], after[0])
    o[15] = f[15] - 0.5 * (f[14] + f16)
    o[-1] = jnp.where(is_first, o[1], before[0] - 0.5 * f[0])
    a = {i: f[i] + 0.25 * (o[i - 1] + o[i + 1]) for i in range(0, 16, 2)}
    a16 = jnp.where(is_last, a[12], after[0] + 0.25 * (o[15] + after[1]))
    a[16] = a16
    p = {i: a[i] - 0.5 * (a[i - 2] + a[i + 2]) for i in range(2, 16, 4)}
    p[-2] = jnp.where(is_first, p[2], before[1] + 0.25 * o[-1] - 0.5 * a[0])
    b = {i: a[i] + 0.25 * (p[i - 2] + p[i + 2]) for i in range(0, 16, 4)}
    b[16] = jnp.where(is_last, b[8], a16 + 0.25 * (p[14] + after[2] - 0.5 * a16))
    d4 = b[4] - 0.5 * (b[0] + b[8])
    d12 = b[12] - 0.5 * (b[8] + b[16])
    dm4 = jnp.where(is_first, d4, before[2] + 0.25 * p[-2] - 0.5 * b[0])
    out = {i: o[i] for i in range(1, 16, 2)}
    out.update({i: p[i] for i in range(2, 16, 4)})
    out[4], out[12] = d4, d12
    out[0] = b[0] + 0.25 * (dm4 + d4)
    out[8] = b[8] + 0.25 * (d4 + d12)
    return out


def exchange_kernel(x_ref, o_ref, sums_ref, held, from_before, from_after, to_before, to_after,
                    f_send, f_recv, f_own, h_send, h_recv, r_send, r_recv, r_own):
    frames, phases, inner, width = x_ref.shape
    part = inner // GROUP
    me = lax.axis_index("frame")
    count = lax.axis_size("frame")
    member = me % GROUP
    base = me - member
    is_first = base == 0
    is_last = base == count - GROUP
    previous = (me + count - GROUP) % count
    following = (me + GROUP) % count
    peers = [base + (member + k) % GROUP for k in range(1, GROUP)]

    barrier = pltpu.get_barrier_semaphore()
    for peer in peers + [previous, following]:
        pl.semaphore_signal(barrier, inc=1, device_id={"frame": peer}, device_id_type=MESH)
    pl.semaphore_wait(barrier, GROUP + 1)

    def part_of(device):
        return pl.ds(pl.multiple_of((device % GROUP) * part, 8), part)

    def frames_of(device):
        return pl.ds((device % GROUP) * frames, frames)

    def forward(c, k):
        peer = peers[k]
        return pltpu.make_async_remote_copy(
            src_ref=x_ref.at[:, c, part_of(peer), :],
            dst_ref=held.at[frames_of(me), c],
            send_sem=f_send.at[k, c],
            recv_sem=f_recv.at[k, c],
            device_id={"frame": peer},
            device_id_type=MESH,
        )

    def forward_own(c):
        return pltpu.make_async_copy(
            x_ref.at[:, c, part_of(me), :], held.at[frames_of(me), c], f_own.at[c]
        )

    def halo(c, side):
        return pltpu.make_async_remote_copy(
            src_ref=(to_before if side == 0 else to_after).at[c],
            dst_ref=(from_after if side == 0 else from_before).at[c],
            send_sem=h_send.at[side, c],
            recv_sem=h_recv.at[side, c],
            device_id={"frame": previous if side == 0 else following},
            device_id_type=MESH,
        )

    def back(c, k):
        peer = peers[k]
        return pltpu.make_async_remote_copy(
            src_ref=held.at[frames_of(peer), c],
            dst_ref=o_ref.at[:, c, part_of(me), :],
            send_sem=r_send.at[k, c],
            recv_sem=r_recv.at[k, c],
            device_id={"frame": peer},
            device_id_type=MESH,
        )

    def back_own(c):
        return pltpu.make_async_copy(
            held.at[frames_of(me), c], o_ref.at[:, c, part_of(me), :], r_own.at[c]
        )

    def start_forward(c, carry):
        for k in range(GROUP - 1):
            forward(c, k).start()
        forward_own(c).start()
        return carry

    lax.fori_loop(0, phases, start_forward, 0)
    total = GROUP * frames
    strip = 128
    strips = width // strip

    def send_halo(c):
        for k in range(GROUP - 1):
            forward(c, k).wait_recv()
        forward_own(c).wait()

        def tile(i, carry):
            lanes = pl.ds(pl.multiple_of(i * strip, strip), strip)
            left, right = outgoing([held[n, c, :, lanes] for n in range(total)])
            for j in range(TLEVELS):
                to_before[c, j, :, lanes] = left[j]
                to_after[c, j, :, lanes] = right[j]
            return carry

        lax.fori_loop(0, strips, tile, 0)
        for side in range(2):
            halo(c, side).start()

    def finish(c):
        for side in range(2):
            halo(c, side).wait_recv()

        def tile(i, carry):
            lanes = pl.ds(pl.multiple_of(i * strip, strip), strip)
            f = [held[n, c, :, lanes] for n in range(total)]
            before = [from_before[c, j, :, lanes] for j in range(TLEVELS)]
            after = [from_after[c, j, :, lanes] for j in range(TLEVELS)]
            out = temporal(f, before, after, is_first, is_last)
            sums = [None] * (TLEVELS + 1)
            for n in range(total):
                held[n, c, :, lanes] = out[n]
                t = level_of(n % 2**TLEVELS, TLEVELS) - 1
                square = out[n] * out[n]
                sums[t] = square if sums[t] is None else sums[t] + square
            for t in range(TLEVELS + 1):
                sums_ref[t, c, :, lanes] = jnp.sum(
                    sums[t].reshape(part // 8, 8, strip), axis=0
                )
            return carry

        lax.fori_loop(0, strips, tile, 0)
        for k in range(GROUP - 1):
            back(c, k).start()
        back_own(c).start()

    send_halo(0)

    def middle(c, carry):
        send_halo(c)
        finish(c - 1)
        return carry

    lax.fori_loop(1, phases, middle, 0)
    finish(phases - 1)

    def drain(c, carry):
        for k in range(GROUP - 1):
            forward(c, k).wait_send()
            back(c, k).wait()
        for side in range(2):
            halo(c, side).wait_send()
        back_own(c).wait()
        return carry

    lax.fori_loop(0, phases, drain, 0)


def exchange(planes):
    frames, phases, inner, width = planes.shape
    part = inner // GROUP
    any_space = pl.BlockSpec(memory_space=pl.ANY)
    halo_buffer = pltpu.VMEM((phases, TLEVELS, part, width), jnp.float32)
    dma = pltpu.SemaphoreType.DMA
    return pl.pallas_call(
        exchange_kernel,
        out_shape=(
            jax.ShapeDtypeStruct(planes.shape, jnp.float32),
            jax.ShapeDtypeStruct((TLEVELS + 1, phases, 8, width), jnp.float32),
        ),
        in_specs=[any_space],
        out_specs=(any_space, pl.BlockSpec(memory_space=pltpu.VMEM)),
        scratch_shapes=[
            pltpu.VMEM((GROUP * frames, phases, part, width), jnp.float32),
            halo_buffer, halo_buffer, halo_buffer, halo_buffer,
            dma((GROUP - 1, phases)), dma((GROUP - 1, phases)), dma((phases,)),
            dma((2, phases)), dma((2, phases)),
            dma((GROUP - 1, phases)), dma((GROUP - 1, phases)), dma((phases,)),
        ],
        compiler_params=pltpu.CompilerParams(
            collective_id=0, has_side_effects=True, vmem_limit_bytes=50 * 2**20
        ),
    )(planes)


def shards(footage):
    frames, rows, width = footage.shape
    planes = spatial(footage)
    coeffs, sums = exchange(planes)
    coeffs = coeffs.transpose(0, 2, 1, 3).reshape(frames, rows, width)
    pattern = sums.sum(axis=2).reshape(TLEVELS + 1, PERIOD, width // PERIOD, PERIOD).sum(axis=2)
    pattern = pattern.reshape(TLEVELS + 1, PERIOD * PERIOD)
    totals = jnp.dot(
        pattern, jnp.asarray(space_table(SLEVELS), jnp.float32), precision=lax.Precision.HIGHEST
    )
    totals = lax.psum(totals, ("frame", "row"))
    means = band_means(
        totals,
        frames * lax.axis_size("frame"),
        rows * lax.axis_size("row"),
        width,
        SLEVELS,
        TLEVELS,
    )
    return (coeffs, means)


def solution(mesh):
    return jax.shard_map(
        shards,
        mesh=mesh,
        in_specs=(P("frame", "row", None),),
        out_specs=(P("frame", "row", None), P()),
        check_vma=False,
    )
```

```python
import functools

import jax
import jax.numpy as jnp
import numpy as np
from jax import lax
from jax.experimental import pallas as pl
from jax.experimental.pallas import tpu as pltpu
from jax.sharding import PartitionSpec as P

SLEVELS = 3
TLEVELS = 3
PERIOD = 2**SLEVELS
MARGIN = 4
GROUP = 4

LIFT_ALPHA = -1.586134342
LIFT_BETA = -0.05298011854
LIFT_GAMMA = 0.8829110762
LIFT_DELTA = 0.4435068522
LIFT_ZETA = 1.149604398
STEPS = (LIFT_ALPHA, LIFT_BETA, LIFT_GAMMA, LIFT_DELTA)
REACH = 4
TAPS = 2 * REACH + 1
MASKS = TAPS * SLEVELS
MESH = pl.DeviceIdType.MESH


def level_of(number, ceiling):
    depth_now = 1
    while number % 2 == 0 and depth_now <= ceiling:
        number = number // 2
        depth_now = depth_now + 1
    return depth_now


def space_table(levels):
    period = 2**levels
    band_table = np.zeros((period * period, 3 * levels + 1), np.float32)
    for row_pos in range(period):
        for col_pos in range(period):
            row_level = level_of(row_pos, levels)
            col_level = level_of(col_pos, levels)
            finest = min(row_level, col_level)
            if finest > levels:
                column = 3 * levels
            elif row_level == col_level:
                column = 3 * (finest - 1) + 2
            elif row_level == finest:
                column = 3 * (finest - 1)
            else:
                column = 3 * (finest - 1) + 1
            band_table[row_pos * period + col_pos, column] = 1.0
    return band_table


def time_table(levels):
    period = 2**levels
    band_table = np.zeros((period, levels + 1), np.float32)
    for number in range(period):
        band_table[number, level_of(number, levels) - 1] = 1.0
    return band_table


def band_means(totals, frames_all, rows_all, cols_all, levels_s, levels_t):
    space_share = space_table(levels_s).sum(0) / float((2**levels_s) ** 2)
    time_share = time_table(levels_t).sum(0) / float(2**levels_t)
    counts = (
        float(frames_all) * float(rows_all) * float(cols_all) * np.outer(time_share, space_share)
    )
    return totals / jnp.asarray(counts, jnp.float32)


def shifted(block, axis, distance):
    devices = range(lax.axis_size(axis))
    route = [(i - distance, i) for i in devices if i - distance in devices]
    return lax.ppermute(block, axis, route)


def lifted_identity(size):
    x = np.eye(size)
    after = np.concatenate([np.arange(2, size, 2), [size - 2]])
    before = np.concatenate([[1], np.arange(1, size - 1, 2)])
    even, odd = np.arange(0, size, 2), np.arange(1, size, 2)
    x[:, odd] += LIFT_ALPHA * (x[:, even] + x[:, after])
    x[:, even] += LIFT_BETA * (x[:, before] + x[:, odd])
    x[:, odd] += LIFT_GAMMA * (x[:, even] + x[:, after])
    x[:, even] += LIFT_DELTA * (x[:, before] + x[:, odd])
    x[:, even] *= LIFT_ZETA
    x[:, odd] *= 1.0 / LIFT_ZETA
    return x


def lane_table(width):
    table = np.zeros((MASKS + SLEVELS, width), np.float64)
    for level in range(SLEVELS):
        s = 2**level
        size = width // s
        matrix = lifted_identity(size)
        table[TAPS * level + REACH] = 1.0
        for k in range(-REACH, REACH + 1):
            n = np.arange(max(0, -k), min(size, size - k))
            row = np.zeros(size)
            row[n] = matrix[n + k, n]
            table[TAPS * level + REACH + k, ::s] = row
        table[MASKS + level, ::s] = 1.0
    return table.astype(np.float32)


def spatial_kernel(tab_ref, x_ref, halo_ref, o_ref, xin, buf, x_sem, h_sem):
    groups, width = buf.shape[1:]
    inner = groups - 2 * MARGIN
    row = lax.axis_index("row")
    at_top = row == 0
    at_bottom = row == lax.axis_size("row") - 1
    frame = pl.program_id(0)
    slot = frame % 2

    def copies(f, slot):
        for p in range(PERIOD):
            yield pltpu.make_async_copy(
                x_ref.at[f, :, p, :], xin.at[slot, p, pl.ds(0, inner), :], x_sem.at[slot, p]
            )
            yield pltpu.make_async_copy(
                halo_ref.at[f, p], xin.at[slot, p, pl.ds(inner, 2 * MARGIN), :], h_sem.at[slot, p]
            )

    @pl.when(frame == 0)
    def _():
        for copy in copies(frame, slot):
            copy.start()

    @pl.when(frame + 1 < pl.num_programs(0))
    def _():
        for copy in copies(frame + 1, 1 - slot):
            copy.start()

    for copy in copies(frame, slot):
        copy.wait()

    tile = 24
    tiles = groups // tile
    for level in range(SLEVELS):
        s = 2**level
        source = xin.at[slot] if level == 0 else buf

        def columns(i, carry, level=level, s=s, source=source):
            phase = (i // tiles) * s
            q = pl.ds(pl.multiple_of((i % tiles) * tile, 8), tile)
            x = source[phase, q, :]
            y = x * tab_ref[pl.ds(TAPS * level + REACH, 1), :]
            for k in range(1, REACH + 1):
                for sign in (-1, 1):
                    moved = pltpu.roll(x, (-sign * k * s) % width, 1)
                    y = y + moved * tab_ref[pl.ds(TAPS * level + REACH + sign * k, 1), :]
            buf[phase, q, :] = y
            return carry

        lax.fori_loop(0, (PERIOD // s) * tiles, columns, 0)

        def rows(i, carry, level=level, s=s):
            lanes = pl.ds(pl.multiple_of(i * 128, 128), 128)
            mask = tab_ref[pl.ds(MASKS + level, 1), lanes]
            x = {p: buf[p, :, lanes] for p in range(0, PERIOD, s)}
            index = lax.broadcasted_iota(jnp.int32, (groups, 128), 0)
            first = jnp.logical_and(index == 0, at_top)
            last = jnp.logical_and(index == inner - 1, at_bottom)
            for step, factor in enumerate(STEPS):
                c = factor * mask
                if step % 2 == 0:
                    for p in range(s, PERIOD, 2 * s):
                        if p + s < PERIOD:
                            after = x[p + s]
                        else:
                            after = jnp.where(last, x[p - s], pltpu.roll(x[0], groups - 1, 0))
                        x[p] = x[p] + c * (x[p - s] + after)
                else:
                    for p in range(0, PERIOD, 2 * s):
                        if p > 0:
                            before = x[p - s]
                        else:
                            before = jnp.where(first, x[s], pltpu.roll(x[PERIOD - s], 1, 0))
                        x[p] = x[p] + c * (before + x[p + s])
            up = jnp.where(mask > 0, LIFT_ZETA, 1.0)
            down = jnp.where(mask > 0, 1.0 / LIFT_ZETA, 1.0)
            for p in x:
                low = p % (2 * s) == 0
                value = x[p] * (up if low else down)
                if low and level < SLEVELS - 1:
                    buf[p, :, lanes] = value
                else:
                    o_ref[0, p, :, lanes] = value[:inner]
            return carry

        lax.fori_loop(0, width // 128, rows, 0)


def spatial(footage):
    frames, rows, width = footage.shape
    edge = MARGIN * PERIOD
    inner = rows // PERIOD
    groups = inner + 2 * MARGIN
    above = shifted(footage[:, -edge:], "row", 1)
    below = shifted(footage[:, :edge], "row", -1)
    halo = jnp.concatenate([below, above], axis=1)
    halo = halo.reshape(frames, 2 * MARGIN, PERIOD, width).transpose(0, 2, 1, 3)
    table = jnp.asarray(lane_table(width))
    any_space = pl.BlockSpec(memory_space=pl.ANY)
    return pl.pallas_call(
        spatial_kernel,
        grid=(frames,),
        out_shape=jax.ShapeDtypeStruct((frames, PERIOD, inner, width), jnp.float32),
        in_specs=[pl.BlockSpec(table.shape, lambda i: (0, 0)), any_space, any_space],
        out_specs=pl.BlockSpec((1, PERIOD, inner, width), lambda i: (i, 0, 0, 0)),
        scratch_shapes=[
            pltpu.VMEM((2, PERIOD, groups, width), jnp.float32),
            pltpu.VMEM((PERIOD, groups, width), jnp.float32),
            pltpu.SemaphoreType.DMA((2, PERIOD)),
            pltpu.SemaphoreType.DMA((2, PERIOD)),
        ],
        compiler_params=pltpu.CompilerParams(vmem_limit_bytes=50 * 2**20),
    )(table, footage.reshape(frames, inner, PERIOD, width), halo)


def outgoing(f):
    o = {i: f[i] - 0.5 * (f[i - 1] + f[i + 1]) for i in range(1, 14, 2)}
    a = {i: f[i] + 0.25 * (o[i - 1] + o[i + 1]) for i in range(2, 13, 2)}
    p6 = a[6] - 0.5 * (a[4] + a[8])
    p10 = a[10] - 0.5 * (a[8] + a[12])
    b8 = a[8] + 0.25 * (p6 + p10)
    to_before = (f[0], o[1], a[2] - 0.5 * a[4])
    to_after = (
        f[15] - 0.5 * f[14],
        f[14] + 0.25 * o[13] - 0.5 * a[12],
        a[12] + 0.25 * p10 - 0.5 * b8,
    )
    return to_before, to_after


def temporal(f, before, after, is_first, is_last):
    o = {i: f[i] - 0.5 * (f[i - 1] + f[i + 1]) for i in range(1, 14, 2)}
    f16 = jnp.where(is_last, f[14], after[0])
    o[15] = f[15] - 0.5 * (f[14] + f16)
    o[-1] = jnp.where(is_first, o[1], before[0] - 0.5 * f[0])
    a = {i: f[i] + 0.25 * (o[i - 1] + o[i + 1]) for i in range(0, 16, 2)}
    a16 = jnp.where(is_last, a[12], after[0] + 0.25 * (o[15] + after[1]))
    a[16] = a16
    p = {i: a[i] - 0.5 * (a[i - 2] + a[i + 2]) for i in range(2, 16, 4)}
    p[-2] = jnp.where(is_first, p[2], before[1] + 0.25 * o[-1] - 0.5 * a[0])
    b = {i: a[i] + 0.25 * (p[i - 2] + p[i + 2]) for i in range(0, 16, 4)}
    b[16] = jnp.where(is_last, b[8], a16 + 0.25 * (p[14] + after[2] - 0.5 * a16))
    d4 = b[4] - 0.5 * (b[0] + b[8])
    d12 = b[12] - 0.5 * (b[8] + b[16])
    dm4 = jnp.where(is_first, d4, before[2] + 0.25 * p[-2] - 0.5 * b[0])
    out = {i: o[i] for i in range(1, 16, 2)}
    out.update({i: p[i] for i in range(2, 16, 4)})
    out[4], out[12] = d4, d12
    out[0] = b[0] + 0.25 * (dm4 + d4)
    out[8] = b[8] + 0.25 * (d4 + d12)
    return out


def exchange_kernel(x_ref, o_ref, sums_ref, held, from_before, from_after, to_before, to_after,
                    f_send, f_recv, f_own, h_send, h_recv, r_send, r_recv, r_own):
    frames, phases, inner, width = x_ref.shape
    part = inner // GROUP
    me = lax.axis_index("frame")
    count = lax.axis_size("frame")
    member = me % GROUP
    base = me - member
    is_first = base == 0
    is_last = base == count - GROUP
    previous = (me + count - GROUP) % count
    following = (me + GROUP) % count
    peers = [base + (member + k) % GROUP for k in range(1, GROUP)]

    barrier = pltpu.get_barrier_semaphore()
    for peer in peers + [previous, following]:
        pl.semaphore_signal(barrier, inc=1, device_id={"frame": peer}, device_id_type=MESH)
    pl.semaphore_wait(barrier, GROUP + 1)

    def part_of(device):
        return pl.ds(pl.multiple_of((device % GROUP) * part, 8), part)

    def frames_of(device):
        return pl.ds((device % GROUP) * frames, frames)

    def forward(c, k):
        peer = peers[k]
        return pltpu.make_async_remote_copy(
            src_ref=x_ref.at[:, c, part_of(peer), :],
            dst_ref=held.at[frames_of(me), c],
            send_sem=f_send.at[k, c],
            recv_sem=f_recv.at[k, c],
            device_id={"frame": peer},
            device_id_type=MESH,
        )

    def forward_own(c):
        return pltpu.make_async_copy(
            x_ref.at[:, c, part_of(me), :], held.at[frames_of(me), c], f_own.at[c]
        )

    def halo(c, side):
        return pltpu.make_async_remote_copy(
            src_ref=(to_before if side == 0 else to_after).at[c],
            dst_ref=(from_after if side == 0 else from_before).at[c],
            send_sem=h_send.at[side, c],
            recv_sem=h_recv.at[side, c],
            device_id={"frame": previous if side == 0 else following},
            device_id_type=MESH,
        )

    def back(c, k):
        peer = peers[k]
        return pltpu.make_async_remote_copy(
            src_ref=held.at[frames_of(peer), c],
            dst_ref=o_ref.at[:, c, part_of(me), :],
            send_sem=r_send.at[k, c],
            recv_sem=r_recv.at[k, c],
            device_id={"frame": peer},
            device_id_type=MESH,
        )

    def back_own(c):
        return pltpu.make_async_copy(
            held.at[frames_of(me), c], o_ref.at[:, c, part_of(me), :], r_own.at[c]
        )

    def start_forward(c, carry):
        for k in range(GROUP - 1):
            forward(c, k).start()
        forward_own(c).start()
        return carry

    lax.fori_loop(0, phases, start_forward, 0)
    total = GROUP * frames
    strip = 128
    strips = width // strip

    def send_halo(c):
        for k in range(GROUP - 1):
            forward(c, k).wait_recv()
        forward_own(c).wait()

        def tile(i, carry):
            lanes = pl.ds(pl.multiple_of(i * strip, strip), strip)
            left, right = outgoing([held[n, c, :, lanes] for n in range(total)])
            for j in range(TLEVELS):
                to_before[c, j, :, lanes] = left[j]
                to_after[c, j, :, lanes] = right[j]
            return carry

        lax.fori_loop(0, strips, tile, 0)
        for side in range(2):
            halo(c, side).start()

    def finish(c):
        for side in range(2):
            halo(c, side).wait_recv()

        def tile(i, carry):
            lanes = pl.ds(pl.multiple_of(i * strip, strip), strip)
            f = [held[n, c, :, lanes] for n in range(total)]
            before = [from_before[c, j, :, lanes] for j in range(TLEVELS)]
            after = [from_after[c, j, :, lanes] for j in range(TLEVELS)]
            out = temporal(f, before, after, is_first, is_last)
            sums = [None] * (TLEVELS + 1)
            for n in range(total):
                held[n, c, :, lanes] = out[n]
                t = level_of(n % 2**TLEVELS, TLEVELS) - 1
                square = out[n] * out[n]
                sums[t] = square if sums[t] is None else sums[t] + square
            for t in range(TLEVELS + 1):
                sums_ref[t, c, :, lanes] = jnp.sum(
                    sums[t].reshape(part // 8, 8, strip), axis=0
                )
            return carry

        lax.fori_loop(0, strips, tile, 0)
        for k in range(GROUP - 1):
            back(c, k).start()
        back_own(c).start()

    send_halo(0)

    def middle(c, carry):
        send_halo(c)
        finish(c - 1)
        return carry

    lax.fori_loop(1, phases, middle, 0)
    finish(phases - 1)

    def drain(c, carry):
        for k in range(GROUP - 1):
            forward(c, k).wait_send()
            back(c, k).wait()
        for side in range(2):
            halo(c, side).wait_send()
        back_own(c).wait()
        return carry

    lax.fori_loop(0, phases, drain, 0)


def exchange(planes):
    frames, phases, inner, width = planes.shape
    part = inner // GROUP
    any_space = pl.BlockSpec(memory_space=pl.ANY)
    halo_buffer = pltpu.VMEM((phases, TLEVELS, part, width), jnp.float32)
    dma = pltpu.SemaphoreType.DMA
    return pl.pallas_call(
        exchange_kernel,
        out_shape=(
            jax.ShapeDtypeStruct(planes.shape, jnp.float32),
            jax.ShapeDtypeStruct((TLEVELS + 1, phases, 8, width), jnp.float32),
        ),
        in_specs=[any_space],
        out_specs=(any_space, pl.BlockSpec(memory_space=pltpu.VMEM)),
        scratch_shapes=[
            pltpu.VMEM((GROUP * frames, phases, part, width), jnp.float32),
            halo_buffer, halo_buffer, halo_buffer, halo_buffer,
            dma((GROUP - 1, phases)), dma((GROUP - 1, phases)), dma((phases,)),
            dma((2, phases)), dma((2, phases)),
            dma((GROUP - 1, phases)), dma((GROUP - 1, phases)), dma((phases,)),
        ],
        compiler_params=pltpu.CompilerParams(
            collective_id=0, has_side_effects=True, vmem_limit_bytes=50 * 2**20
        ),
    )(planes)


def total_kernel(x_ref, o_ref, inbox, send, recv):
    strips = lax.axis_size("row")
    count = lax.axis_size("frame") * strips
    me = lax.axis_index("frame") * strips + lax.axis_index("row")

    def place(device):
        return {"frame": device // strips, "row": device % strips}

    barrier = pltpu.get_barrier_semaphore()

    def greet(j, carry):
        pl.semaphore_signal(
            barrier, inc=1, device_id=place((me + j) % count), device_id_type=MESH
        )
        return carry

    lax.fori_loop(1, count, greet, 0)
    pl.semaphore_wait(barrier, count - 1)

    def to_peer(j):
        return pltpu.make_async_remote_copy(
            src_ref=x_ref,
            dst_ref=inbox.at[me],
            send_sem=send.at[j],
            recv_sem=recv.at[me],
            device_id=place((me + j) % count),
            device_id_type=MESH,
        )

    def start(j, carry):
        to_peer(j).start()
        return carry

    lax.fori_loop(1, count, start, 0)

    inbox[me] = x_ref[...]

    def arrive(j, carry):
        source = (me + j) % count
        pltpu.make_async_remote_copy(
            src_ref=x_ref,
            dst_ref=inbox.at[source],
            send_sem=send.at[j],
            recv_sem=recv.at[source],
            device_id=place(source),
            device_id_type=MESH,
        ).wait_recv()
        return carry

    lax.fori_loop(1, count, arrive, 0)
    o_ref[...] = lax.fori_loop(
        1, count, lambda j, total: total + inbox[j], inbox[0]
    )

    def drain(j, carry):
        to_peer(j).wait_send()
        return carry

    lax.fori_loop(1, count, drain, 0)


def total_over_devices(values):
    count = lax.axis_size("frame") * lax.axis_size("row")
    padded = jnp.zeros((8, 128), jnp.float32)
    padded = padded.at[: values.shape[0], : values.shape[1]].set(values)
    vmem = pl.BlockSpec(memory_space=pltpu.VMEM)
    total = pl.pallas_call(
        total_kernel,
        out_shape=jax.ShapeDtypeStruct((8, 128), jnp.float32),
        in_specs=[vmem],
        out_specs=vmem,
        scratch_shapes=[
            pltpu.VMEM((count, 8, 128), jnp.float32),
            pltpu.SemaphoreType.DMA((count,)),
            pltpu.SemaphoreType.DMA((count,)),
        ],
        compiler_params=pltpu.CompilerParams(collective_id=1, has_side_effects=True),
    )(padded)
    return total[: values.shape[0], : values.shape[1]]


def shards(footage):
    frames, rows, width = footage.shape
    planes = spatial(footage)
    coeffs, sums = exchange(planes)
    coeffs = coeffs.transpose(0, 2, 1, 3).reshape(frames, rows, width)
    pattern = sums.sum(axis=2).reshape(TLEVELS + 1, PERIOD, width // PERIOD, PERIOD).sum(axis=2)
    pattern = pattern.reshape(TLEVELS + 1, PERIOD * PERIOD)
    totals = jnp.dot(
        pattern, jnp.asarray(space_table(SLEVELS), jnp.float32), precision=lax.Precision.HIGHEST
    )
    totals = total_over_devices(totals)
    means = band_means(
        totals,
        frames * lax.axis_size("frame"),
        rows * lax.axis_size("row"),
        width,
        SLEVELS,
        TLEVELS,
    )
    return (coeffs, means)


def solution(mesh):
    return jax.shard_map(
        shards,
        mesh=mesh,
        in_specs=(P("frame", "row", None),),
        out_specs=(P("frame", "row", None), P()),
        check_vma=False,
    )
```

```python
import functools

import jax
import jax.numpy as jnp
import numpy as np
from jax import lax
from jax.experimental import pallas as pl
from jax.experimental.pallas import tpu as pltpu
from jax.sharding import PartitionSpec as P

SLEVELS = 3
TLEVELS = 3
PERIOD = 2**SLEVELS
MARGIN = 4
GROUP = 4

LIFT_ALPHA = -1.586134342
LIFT_BETA = -0.05298011854
LIFT_GAMMA = 0.8829110762
LIFT_DELTA = 0.4435068522
LIFT_ZETA = 1.149604398
STEPS = (LIFT_ALPHA, LIFT_BETA, LIFT_GAMMA, LIFT_DELTA)
REACH = 4
TAPS = 2 * REACH + 1
MASKS = TAPS * SLEVELS
MESH = pl.DeviceIdType.MESH


def level_of(number, ceiling):
    depth_now = 1
    while number % 2 == 0 and depth_now <= ceiling:
        number = number // 2
        depth_now = depth_now + 1
    return depth_now


def space_table(levels):
    period = 2**levels
    band_table = np.zeros((period * period, 3 * levels + 1), np.float32)
    for row_pos in range(period):
        for col_pos in range(period):
            row_level = level_of(row_pos, levels)
            col_level = level_of(col_pos, levels)
            finest = min(row_level, col_level)
            if finest > levels:
                column = 3 * levels
            elif row_level == col_level:
                column = 3 * (finest - 1) + 2
            elif row_level == finest:
                column = 3 * (finest - 1)
            else:
                column = 3 * (finest - 1) + 1
            band_table[row_pos * period + col_pos, column] = 1.0
    return band_table


def time_table(levels):
    period = 2**levels
    band_table = np.zeros((period, levels + 1), np.float32)
    for number in range(period):
        band_table[number, level_of(number, levels) - 1] = 1.0
    return band_table


def band_means(totals, frames_all, rows_all, cols_all, levels_s, levels_t):
    space_share = space_table(levels_s).sum(0) / float((2**levels_s) ** 2)
    time_share = time_table(levels_t).sum(0) / float(2**levels_t)
    counts = (
        float(frames_all) * float(rows_all) * float(cols_all) * np.outer(time_share, space_share)
    )
    return totals / jnp.asarray(counts, jnp.float32)


def shifted(block, axis, distance):
    devices = range(lax.axis_size(axis))
    route = [(i - distance, i) for i in devices if i - distance in devices]
    return lax.ppermute(block, axis, route)


def lifted_identity(size):
    x = np.eye(size)
    after = np.concatenate([np.arange(2, size, 2), [size - 2]])
    before = np.concatenate([[1], np.arange(1, size - 1, 2)])
    even, odd = np.arange(0, size, 2), np.arange(1, size, 2)
    x[:, odd] += LIFT_ALPHA * (x[:, even] + x[:, after])
    x[:, even] += LIFT_BETA * (x[:, before] + x[:, odd])
    x[:, odd] += LIFT_GAMMA * (x[:, even] + x[:, after])
    x[:, even] += LIFT_DELTA * (x[:, before] + x[:, odd])
    x[:, even] *= LIFT_ZETA
    x[:, odd] *= 1.0 / LIFT_ZETA
    return x


def lane_table(width):
    table = np.zeros((MASKS + SLEVELS, width), np.float64)
    for level in range(SLEVELS):
        s = 2**level
        size = width // s
        matrix = lifted_identity(size)
        table[TAPS * level + REACH] = 1.0
        for k in range(-REACH, REACH + 1):
            n = np.arange(max(0, -k), min(size, size - k))
            row = np.zeros(size)
            row[n] = matrix[n + k, n]
            table[TAPS * level + REACH + k, ::s] = row
        table[MASKS + level, ::s] = 1.0
    return table.astype(np.float32)


def spatial_frame(frame, frames, tab_ref, x_ref, halo_ref, o_ref, xin, buf, x_sem, h_sem):
    groups, width = buf.shape[1:]
    inner = groups - 2 * MARGIN
    row = lax.axis_index("row")
    at_top = row == 0
    at_bottom = row == lax.axis_size("row") - 1
    slot = frame % 2

    def copies(f, slot):
        for p in range(PERIOD):
            yield pltpu.make_async_copy(
                x_ref.at[f, :, p, :], xin.at[slot, p, pl.ds(0, inner), :], x_sem.at[slot, p]
            )
            yield pltpu.make_async_copy(
                halo_ref.at[f, p], xin.at[slot, p, pl.ds(inner, 2 * MARGIN), :], h_sem.at[slot, p]
            )

    @pl.when(frame == 0)
    def _():
        for copy in copies(frame, slot):
            copy.start()

    @pl.when(frame + 1 < frames)
    def _():
        for copy in copies(frame + 1, 1 - slot):
            copy.start()

    for copy in copies(frame, slot):
        copy.wait()

    tile = 24
    tiles = groups // tile
    for level in range(SLEVELS):
        s = 2**level
        source = xin.at[slot] if level == 0 else buf

        def columns(i, carry, level=level, s=s, source=source):
            phase = (i // tiles) * s
            q = pl.ds(pl.multiple_of((i % tiles) * tile, 8), tile)
            x = source[phase, q, :]
            y = x * tab_ref[pl.ds(TAPS * level + REACH, 1), :]
            for k in range(1, REACH + 1):
                for sign in (-1, 1):
                    moved = pltpu.roll(x, (-sign * k * s) % width, 1)
                    y = y + moved * tab_ref[pl.ds(TAPS * level + REACH + sign * k, 1), :]
            buf[phase, q, :] = y
            return carry

        lax.fori_loop(0, (PERIOD // s) * tiles, columns, 0)

        def rows(i, carry, level=level, s=s):
            lanes = pl.ds(pl.multiple_of(i * 128, 128), 128)
            mask = tab_ref[pl.ds(MASKS + level, 1), lanes]
            x = {p: buf[p, :, lanes] for p in range(0, PERIOD, s)}
            index = lax.broadcasted_iota(jnp.int32, (groups, 128), 0)
            first = jnp.logical_and(index == 0, at_top)
            last = jnp.logical_and(index == inner - 1, at_bottom)
            for step, factor in enumerate(STEPS):
                c = factor * mask
                if step % 2 == 0:
                    for p in range(s, PERIOD, 2 * s):
                        if p + s < PERIOD:
                            after = x[p + s]
                        else:
                            after = jnp.where(last, x[p - s], pltpu.roll(x[0], groups - 1, 0))
                        x[p] = x[p] + c * (x[p - s] + after)
                else:
                    for p in range(0, PERIOD, 2 * s):
                        if p > 0:
                            before = x[p - s]
                        else:
                            before = jnp.where(first, x[s], pltpu.roll(x[PERIOD - s], 1, 0))
                        x[p] = x[p] + c * (before + x[p + s])
            up = jnp.where(mask > 0, LIFT_ZETA, 1.0)
            down = jnp.where(mask > 0, 1.0 / LIFT_ZETA, 1.0)
            for p in x:
                low = p % (2 * s) == 0
                value = x[p] * (up if low else down)
                if low and level < SLEVELS - 1:
                    buf[p, :, lanes] = value
                else:
                    o_ref[frame, p, :, lanes] = value[:inner]
            return carry

        lax.fori_loop(0, width // 128, rows, 0)


def outgoing(f):
    o = {i: f[i] - 0.5 * (f[i - 1] + f[i + 1]) for i in range(1, 14, 2)}
    a = {i: f[i] + 0.25 * (o[i - 1] + o[i + 1]) for i in range(2, 13, 2)}
    p6 = a[6] - 0.5 * (a[4] + a[8])
    p10 = a[10] - 0.5 * (a[8] + a[12])
    b8 = a[8] + 0.25 * (p6 + p10)
    to_before = (f[0], o[1], a[2] - 0.5 * a[4])
    to_after = (
        f[15] - 0.5 * f[14],
        f[14] + 0.25 * o[13] - 0.5 * a[12],
        a[12] + 0.25 * p10 - 0.5 * b8,
    )
    return to_before, to_after


def temporal(f, before, after, is_first, is_last):
    o = {i: f[i] - 0.5 * (f[i - 1] + f[i + 1]) for i in range(1, 14, 2)}
    f16 = jnp.where(is_last, f[14], after[0])
    o[15] = f[15] - 0.5 * (f[14] + f16)
    o[-1] = jnp.where(is_first, o[1], before[0] - 0.5 * f[0])
    a = {i: f[i] + 0.25 * (o[i - 1] + o[i + 1]) for i in range(0, 16, 2)}
    a16 = jnp.where(is_last, a[12], after[0] + 0.25 * (o[15] + after[1]))
    a[16] = a16
    p = {i: a[i] - 0.5 * (a[i - 2] + a[i + 2]) for i in range(2, 16, 4)}
    p[-2] = jnp.where(is_first, p[2], before[1] + 0.25 * o[-1] - 0.5 * a[0])
    b = {i: a[i] + 0.25 * (p[i - 2] + p[i + 2]) for i in range(0, 16, 4)}
    b[16] = jnp.where(is_last, b[8], a16 + 0.25 * (p[14] + after[2] - 0.5 * a16))
    d4 = b[4] - 0.5 * (b[0] + b[8])
    d12 = b[12] - 0.5 * (b[8] + b[16])
    dm4 = jnp.where(is_first, d4, before[2] + 0.25 * p[-2] - 0.5 * b[0])
    out = {i: o[i] for i in range(1, 16, 2)}
    out.update({i: p[i] for i in range(2, 16, 4)})
    out[4], out[12] = d4, d12
    out[0] = b[0] + 0.25 * (dm4 + d4)
    out[8] = b[8] + 0.25 * (d4 + d12)
    return out


def video_kernel(tab_ref, x_ref, halo_ref, o_ref, sums_ref, xin, buf, planes, mine, held,
                 from_before, from_after, to_before, to_after, x_sem, e_sem,
                 f_send, f_recv, f_own, h_send, h_recv, r_send, r_recv, r_own, m_own):
    frames, phases, inner, width = planes.shape
    part = inner // GROUP
    inside = [n for n in range(1, frames - 1, 2)]
    moved = [n for n in range(frames) if n not in inside]
    me = lax.axis_index("frame")
    count = lax.axis_size("frame")
    member = me % GROUP
    base = me - member
    is_first = base == 0
    is_last = base == count - GROUP
    previous = (me + count - GROUP) % count
    following = (me + GROUP) % count
    peers = [base + (member + k) % GROUP for k in range(1, GROUP)]

    barrier = pltpu.get_barrier_semaphore()
    for peer in peers + [previous, following]:
        pl.semaphore_signal(barrier, inc=1, device_id={"frame": peer}, device_id_type=MESH)
    pl.semaphore_wait(barrier, GROUP + 1)

    def part_of(device):
        return pl.ds(pl.multiple_of((device % GROUP) * part, 8), part)

    def spot(device, n):
        return (device % GROUP) * frames + n

    def forward(n, c, k):
        peer = peers[k]
        return pltpu.make_async_remote_copy(
            src_ref=planes.at[n, c, part_of(peer), :],
            dst_ref=held.at[spot(me, n), c],
            send_sem=f_send.at[n, k, c],
            recv_sem=f_recv.at[n, k, c],
            device_id={"frame": peer},
            device_id_type=MESH,
        )

    def forward_own(n, c):
        return pltpu.make_async_copy(
            planes.at[n, c, part_of(me), :], held.at[spot(me, n), c], f_own.at[n, c]
        )

    def halo(c, side):
        return pltpu.make_async_remote_copy(
            src_ref=(to_before if side == 0 else to_after).at[c],
            dst_ref=(from_after if side == 0 else from_before).at[c],
            send_sem=h_send.at[side, c],
            recv_sem=h_recv.at[side, c],
            device_id={"frame": previous if side == 0 else following},
            device_id_type=MESH,
        )

    def back(i, c, k):
        peer = peers[k]
        return pltpu.make_async_remote_copy(
            src_ref=held.at[spot(peer, moved[i]), c],
            dst_ref=o_ref.at[moved[i], c, part_of(me), :],
            send_sem=r_send.at[i, k, c],
            recv_sem=r_recv.at[i, k, c],
            device_id={"frame": peer},
            device_id_type=MESH,
        )

    def back_own(i, c):
        return pltpu.make_async_copy(
            held.at[spot(me, moved[i]), c], o_ref.at[moved[i], c, part_of(me), :], r_own.at[i, c]
        )

    def keep(i, c):
        return pltpu.make_async_copy(mine.at[i, c], o_ref.at[inside[i], c], m_own.at[i, c])

    def one_frame(n, carry):
        spatial_frame(n, frames, tab_ref, x_ref, halo_ref, planes, xin, buf, x_sem, e_sem)

        def start_forward(c, carry):
            for k in range(GROUP - 1):
                forward(n, c, k).start()
            forward_own(n, c).start()
            return carry

        return lax.fori_loop(0, phases, start_forward, carry)

    lax.fori_loop(0, frames, one_frame, 0)

    def inside_highs(c, carry):
        for i, n in enumerate(inside):
            mine[i, c] = planes[n, c] - 0.5 * (planes[n - 1, c] + planes[n + 1, c])
            keep(i, c).start()
        return carry

    lax.fori_loop(0, phases, inside_highs, 0)
    total = GROUP * frames
    strip = 128
    strips = width // strip

    def send_halo(c):
        for n in range(frames):
            for k in range(GROUP - 1):
                forward(n, c, k).wait_recv()
            forward_own(n, c).wait()

        def tile(i, carry):
            lanes = pl.ds(pl.multiple_of(i * strip, strip), strip)
            left, right = outgoing([held[n, c, :, lanes] for n in range(total)])
            for j in range(TLEVELS):
                to_before[c, j, :, lanes] = left[j]
                to_after[c, j, :, lanes] = right[j]
            return carry

        lax.fori_loop(0, strips, tile, 0)
        for side in range(2):
            halo(c, side).start()

    def finish(c):
        for side in range(2):
            halo(c, side).wait_recv()

        def tile(i, carry):
            lanes = pl.ds(pl.multiple_of(i * strip, strip), strip)
            f = [held[n, c, :, lanes] for n in range(total)]
            before = [from_before[c, j, :, lanes] for j in range(TLEVELS)]
            after = [from_after[c, j, :, lanes] for j in range(TLEVELS)]
            out = temporal(f, before, after, is_first, is_last)
            sums = [None] * (TLEVELS + 1)
            for n in range(total):
                if n % frames in moved:
                    held[n, c, :, lanes] = out[n]
                t = level_of(n % 2**TLEVELS, TLEVELS) - 1
                square = out[n] * out[n]
                sums[t] = square if sums[t] is None else sums[t] + square
            for t in range(TLEVELS + 1):
                sums_ref[t, c, :, lanes] = jnp.sum(
                    sums[t].reshape(part // 8, 8, strip), axis=0
                )
            return carry

        lax.fori_loop(0, strips, tile, 0)
        for i in range(len(moved)):
            for k in range(GROUP - 1):
                back(i, c, k).start()
            back_own(i, c).start()

    send_halo(0)

    def middle(c, carry):
        send_halo(c)
        finish(c - 1)
        return carry

    lax.fori_loop(1, phases, middle, 0)
    finish(phases - 1)

    def drain(c, carry):
        for k in range(GROUP - 1):
            for n in range(frames):
                forward(n, c, k).wait_send()
            for i in range(len(moved)):
                back(i, c, k).wait()
        for side in range(2):
            halo(c, side).wait_send()
        for i in range(len(moved)):
            back_own(i, c).wait()
        for i in range(len(inside)):
            keep(i, c).wait()
        return carry

    lax.fori_loop(0, phases, drain, 0)


def transformed(footage):
    frames, rows, width = footage.shape
    edge = MARGIN * PERIOD
    inner = rows // PERIOD
    groups = inner + 2 * MARGIN
    part = inner // GROUP
    above = shifted(footage[:, -edge:], "row", 1)
    below = shifted(footage[:, :edge], "row", -1)
    halo = jnp.concatenate([below, above], axis=1)
    halo = halo.reshape(frames, 2 * MARGIN, PERIOD, width).transpose(0, 2, 1, 3)
    table = jnp.asarray(lane_table(width))
    any_space = pl.BlockSpec(memory_space=pl.ANY)
    vmem = pl.BlockSpec(memory_space=pltpu.VMEM)
    halo_buffer = pltpu.VMEM((PERIOD, TLEVELS, part, width), jnp.float32)
    dma = pltpu.SemaphoreType.DMA
    kept = len(range(1, frames - 1, 2))
    sent = frames - kept
    return pl.pallas_call(
        video_kernel,
        out_shape=(
            jax.ShapeDtypeStruct((frames, PERIOD, inner, width), jnp.float32),
            jax.ShapeDtypeStruct((TLEVELS + 1, PERIOD, 8, width), jnp.float32),
        ),
        in_specs=[vmem, any_space, any_space],
        out_specs=(any_space, vmem),
        scratch_shapes=[
            pltpu.VMEM((2, PERIOD, groups, width), jnp.float32),
            pltpu.VMEM((PERIOD, groups, width), jnp.float32),
            pltpu.VMEM((frames, PERIOD, inner, width), jnp.float32),
            pltpu.VMEM((kept, PERIOD, inner, width), jnp.float32),
            pltpu.VMEM((GROUP * frames, PERIOD, part, width), jnp.float32),
            halo_buffer, halo_buffer, halo_buffer, halo_buffer,
            dma((2, PERIOD)), dma((2, PERIOD)),
            dma((frames, GROUP - 1, PERIOD)), dma((frames, GROUP - 1, PERIOD)),
            dma((frames, PERIOD)),
            dma((2, PERIOD)), dma((2, PERIOD)),
            dma((sent, GROUP - 1, PERIOD)), dma((sent, GROUP - 1, PERIOD)),
            dma((sent, PERIOD)), dma((kept, PERIOD)),
        ],
        compiler_params=pltpu.CompilerParams(
            collective_id=0, has_side_effects=True, vmem_limit_bytes=56 * 2**20
        ),
    )(table, footage.reshape(frames, inner, PERIOD, width), halo)


def total_kernel(x_ref, o_ref, inbox, send, recv):
    strips = lax.axis_size("row")
    count = lax.axis_size("frame") * strips
    me = lax.axis_index("frame") * strips + lax.axis_index("row")

    def place(device):
        return {"frame": device // strips, "row": device % strips}

    barrier = pltpu.get_barrier_semaphore()

    def greet(j, carry):
        pl.semaphore_signal(
            barrier, inc=1, device_id=place((me + j) % count), device_id_type=MESH
        )
        return carry

    lax.fori_loop(1, count, greet, 0)
    pl.semaphore_wait(barrier, count - 1)

    def to_peer(j):
        return pltpu.make_async_remote_copy(
            src_ref=x_ref,
            dst_ref=inbox.at[me],
            send_sem=send.at[j],
            recv_sem=recv.at[me],
            device_id=place((me + j) % count),
            device_id_type=MESH,
        )

    def start(j, carry):
        to_peer(j).start()
        return carry

    lax.fori_loop(1, count, start, 0)

    inbox[me] = x_ref[...]

    def arrive(j, carry):
        source = (me + j) % count
        pltpu.make_async_remote_copy(
            src_ref=x_ref,
            dst_ref=inbox.at[source],
            send_sem=send.at[j],
            recv_sem=recv.at[source],
            device_id=place(source),
            device_id_type=MESH,
        ).wait_recv()
        return carry

    lax.fori_loop(1, count, arrive, 0)
    o_ref[...] = lax.fori_loop(
        1, count, lambda j, total: total + inbox[j], inbox[0]
    )

    def drain(j, carry):
        to_peer(j).wait_send()
        return carry

    lax.fori_loop(1, count, drain, 0)


def total_over_devices(values):
    count = lax.axis_size("frame") * lax.axis_size("row")
    padded = jnp.zeros((8, 128), jnp.float32)
    padded = padded.at[: values.shape[0], : values.shape[1]].set(values)
    vmem = pl.BlockSpec(memory_space=pltpu.VMEM)
    total = pl.pallas_call(
        total_kernel,
        out_shape=jax.ShapeDtypeStruct((8, 128), jnp.float32),
        in_specs=[vmem],
        out_specs=vmem,
        scratch_shapes=[
            pltpu.VMEM((count, 8, 128), jnp.float32),
            pltpu.SemaphoreType.DMA((count,)),
            pltpu.SemaphoreType.DMA((count,)),
        ],
        compiler_params=pltpu.CompilerParams(collective_id=1, has_side_effects=True),
    )(padded)
    return total[: values.shape[0], : values.shape[1]]


def shards(footage):
    frames, rows, width = footage.shape
    coeffs, sums = transformed(footage)
    coeffs = coeffs.transpose(0, 2, 1, 3).reshape(frames, rows, width)
    pattern = sums.sum(axis=2).reshape(TLEVELS + 1, PERIOD, width // PERIOD, PERIOD).sum(axis=2)
    pattern = pattern.reshape(TLEVELS + 1, PERIOD * PERIOD)
    totals = jnp.dot(
        pattern, jnp.asarray(space_table(SLEVELS), jnp.float32), precision=lax.Precision.HIGHEST
    )
    totals = total_over_devices(totals)
    means = band_means(
        totals,
        frames * lax.axis_size("frame"),
        rows * lax.axis_size("row"),
        width,
        SLEVELS,
        TLEVELS,
    )
    return (coeffs, means)


def solution(mesh):
    return jax.shard_map(
        shards,
        mesh=mesh,
        in_specs=(P("frame", "row", None),),
        out_specs=(P("frame", "row", None), P()),
        check_vma=False,
    )
```
